32 devices in a mesh: dp: 2 (over x), context: 4 (over z), tensor: 4 (over y, core).
Axes of the slice: x: 2, y: 2, z: 4, core: 2. Of those that a mesh axis runs over, the one named last changes fastest.
Arguments:
- queries: bfloat16 [2, 1024, 8192], P('dp', 'context', 'tensor'), may hold values from -45 to 45
- keys: bfloat16 [2, 1024, 1024], P('dp', 'context'), may hold values from -20 to 20
- values: bfloat16 [2, 1024, 1024], P('dp', 'context'), may hold values from -6 to 6
- out_weight: bfloat16 [8192, 8192], P('tensor'), may hold values from -0.0625 to 0.0625
- segment_ids: int32 [2, 1024], P('dp'), may hold values from 0 to 7, as said below
- loss_mask: int32 [2, 1024], P('dp', 'context'), may hold values from 0 to 1, as said below
- span_order: int32 [8], replicated, may hold values from 0 to 7, as said below
Outputs:
- weighted_out: bfloat16 [2, 1024, 8192], P('dp', 'context', 'tensor')
The draws below stay inside these ranges and needn't reach their ends.
Inputs may be any that keep to these rules, and one draw needn't show every extreme that they name: `span_order`: a permutation of 0 .. 7. `segment_ids`: taken in order of sequence position pos (see the steps), a sequence's document numbers never fall; each sequence holds 8 documents. `loss_mask`: the first row of every sequence is 1.
All inputs are finite; a program needn't handle non-finite values.
Results may differ from the reference program's by a relative error of at most 0.018.
Values may be sent and summed in bfloat16 or wider, within the bound.
A program may use at most 128 MiB of HBM per device.

```python
import jax
import jax.numpy as jnp
from jax import lax

D = 8192
QH = 64
KVH = 8
HD = 128
DOCS = 8
TOKENS = 1024
CH = 128
N_DP = 2
N_CONTEXT = 4
N_TENSOR = 4


def paired_heads(key):
    key_first = jax.random.fold_in(key, 11)
    query_first = jax.random.fold_in(key, 12)
    base_keys = jnp.clip(jax.random.normal(key_first, (N_DP, TOKENS, KVH, HD), jnp.float32), -6.0, 6.0)
    base_queries = jnp.clip(jax.random.normal(query_first, (N_DP, TOKENS, QH, HD), jnp.float32), -6.0, 6.0)
    keys_out = base_keys
    queries_out = base_queries
    return (queries_out.reshape(N_DP, TOKENS, QH * HD), keys_out.reshape(N_DP, TOKENS, KVH * HD))


def draw_queries(key, part):
    return paired_heads(key)[0].astype(jnp.bfloat16)


def draw_keys(key, part):
    return paired_heads(key)[1].astype(jnp.bfloat16)


def document_cuts(cut_key):
    chosen = jax.random.permutation(cut_key, TOKENS - 1)[:DOCS - 1].astype(jnp.int32) + 1
    return jnp.zeros((TOKENS,), jnp.int32).at[chosen].set(1)


def layout_tables(key):
    order = jax.random.permutation(jax.random.fold_in(key, 21), 2 * N_CONTEXT).astype(jnp.int32)
    replica_keys = jax.random.split(jax.random.fold_in(key, 22), N_DP)
    starts = jax.vmap(document_cuts)(replica_keys)
    ordered = jnp.cumsum(starts, axis=1).astype(jnp.int32)
    rows = jnp.arange(TOKENS, dtype=jnp.int32)
    position = order[rows // CH] * CH + rows % CH
    return (order, ordered[:, position])


def draw_span_order(key, part):
    return layout_tables(key)[0]


def draw_segment_ids(key, part):
    return layout_tables(key)[1]


def draw_loss_mask(key, part):
    replica = jnp.arange(N_DP, dtype=jnp.int32)[:, None]
    rows = jnp.arange(TOKENS, dtype=jnp.int32)[None, :]
    limit = 150 + 350 * replica // max(N_DP - 1, 1) + 350 * rows // TOKENS
    rolls = jax.random.randint(key, (N_DP, TOKENS), 0, 1000)
    marked = (rolls < limit).astype(jnp.int32)
    return marked.at[:, 0].set(1)


def levels(own_key, shape, cuts, low, largest):
    def one(dim, parts):
        heights = jax.random.uniform(jax.random.fold_in(jax.random.fold_in(own_key, 6), dim), (parts,), jnp.float32, low / len(cuts), largest / len(cuts))
        return jnp.repeat(jnp.exp(heights), shape[dim] // parts).reshape((-1,) + (1,) * (len(shape) - dim - 1))

    gain = one(*cuts[0])
    for cut in cuts[1:]:
        gain = gain * one(*cut)
    return gain


def noise(stream_key, dims, scale, bound, cuts=(), held_as=jnp.bfloat16):
    level = levels(stream_key, dims, cuts, -0.22, 0.18) if cuts else 1.0
    result = jax.random.normal(stream_key, dims, jnp.float32) * scale * level
    return jnp.minimum(jnp.maximum(result, -bound), bound).astype(held_as)


def setup_inputs(seed: int = 0) -> dict:
    key_list = jax.random.split(jax.random.key(seed), 8)
    queries = draw_queries(jax.random.fold_in(key_list[7], 71), 0)
    keys = draw_keys(jax.random.fold_in(key_list[7], 71), 0)
    values = noise(key_list[2], (N_DP, TOKENS, KVH * HD), 1.0, 6.0, ((0, 2), (1, 4)))
    out_weight = noise(key_list[3], (QH * HD, D), (QH * HD) ** -0.5, 0.0625, ((0, 4),))
    segment_ids = draw_segment_ids(jax.random.fold_in(key_list[7], 71), 0)
    loss_mask = draw_loss_mask(jax.random.fold_in(key_list[7], 71), 0)
    span_order = draw_span_order(jax.random.fold_in(key_list[7], 71), 0)
    return {"queries": queries, "keys": keys, "values": values, "out_weight": out_weight, "segment_ids": segment_ids, "loss_mask": loss_mask, "span_order": span_order}


def reference(queries, keys, values, out_weight, segment_ids, loss_mask, span_order):
    rows = jnp.arange(TOKENS, dtype=jnp.int32)
    position = span_order[rows // CH] * CH + rows % CH
    group = QH // KVH
    width = QH * HD // N_TENSOR
    factor = HD ** -0.5
    count = jnp.sum(loss_mask.astype(jnp.float32))
    results = []
    for replica in range(N_DP):
        segment = segment_ids[replica]
        allowed = (segment[:, None] == segment[None, :]) & (position[:, None] >= position[None, :])
        query_all = queries[replica]
        key_all = keys[replica]
        value_all = values[replica]

        def one_head(head):
            query = lax.dynamic_slice_in_dim(query_all, (head * HD).astype(jnp.int32), HD, 1)
            kv_start = ((head // group) * HD).astype(jnp.int32)
            key_head = lax.dynamic_slice_in_dim(key_all, kv_start, HD, 1)
            value_head = lax.dynamic_slice_in_dim(value_all, kv_start, HD, 1)
            scores = jnp.dot(query, key_head.T, preferred_element_type=jnp.float32) * factor
            scores = jnp.where(allowed, scores, -1e30)
            best = jnp.max(scores, axis=-1, keepdims=True)
            probs = jnp.where(allowed, jnp.exp(scores - best), 0.0)
            total = jnp.sum(probs, axis=-1, keepdims=True)
            mixed = jnp.dot(probs.astype(jnp.bfloat16), value_head, preferred_element_type=jnp.float32) / total
            return mixed.astype(jnp.bfloat16)

        heads = lax.map(one_head, jnp.arange(QH, dtype=jnp.int32))
        joined = jnp.transpose(heads, (1, 0, 2)).reshape(TOKENS, QH * HD)
        summed = jnp.zeros((TOKENS, D), jnp.float32)
        for member in range(N_TENSOR):
            partial_value = jnp.dot(joined[:, member * width:(member + 1) * width], out_weight[member * width:(member + 1) * width], preferred_element_type=jnp.float32)
            rounded = lax.optimization_barrier(partial_value.astype(jnp.bfloat16))
            summed = summed + rounded.astype(jnp.float32)
        weight = loss_mask[replica].astype(jnp.float32) * (N_DP * TOKENS) / count
        results.append((summed * weight[:, None]).astype(jnp.bfloat16))
    return jnp.stack(results)
```

```python
import functools

import jax
import jax.numpy as jnp
from jax import lax
from jax.experimental import pallas as pl
from jax.experimental.pallas import tpu as pltpu
from jax.sharding import PartitionSpec as P

QH = 64
KVH = 8
HD = 128
LEAD = 2
HEADS_STEP = 2


def kernel(
    sizes,
    q_hbm,
    k_hbm,
    v_hbm,
    w_hbm,
    seg_ref,
    mask_ref,
    order_ref,
    out_hbm,
    q_buf,
    kv_buf,
    w_buf,
    best_buf,
    acc_buf,
    heads_buf,
    bias_buf,
    masks_buf,
    sib_send,
    sib_recv,
    far_send,
    far_recv,
    own_buf,
    out_buf,
    q_sem,
    kv_load_sem,
    w_sem,
    kv_send_sem,
    kv_recv_sem,
    mask_send_sem,
    mask_recv_sem,
    mask_load_sem,
    sib_send_sem,
    sib_recv_sem,
    far_send_sem,
    far_recv_sem,
    out_sem,
):
    n_dp, n_ctx, n_t = sizes
    rows = q_hbm.shape[1]
    span_rows = rows // 2
    heads_dev = q_hbm.shape[2] // HD
    group = QH // KVH
    kv_dev = kv_buf.shape[1]
    per_kv = heads_dev // kv_dev
    chunk = w_buf.shape[2]
    n_far = n_t // 2
    features = w_hbm.shape[1] // n_t
    per_block = features // chunk
    total = n_far * per_block
    n_masks = n_dp * n_ctx
    factor = HD ** (-0.5)

    dp = lax.axis_index("dp")
    z = lax.axis_index("context")
    t = lax.axis_index("tensor")
    core = lax.rem(t, 2)
    y = lax.div(t, 2)
    sibling = t + 1 - 2 * core
    me = dp * n_ctx + z

    def mask_peer(k):
        index = lax.rem(me + k, n_masks)
        return {"dp": lax.div(index, n_ctx), "context": lax.rem(index, n_ctx), "tensor": t}

    def at(ctx, tensor):
        return {"dp": dp, "context": ctx, "tensor": tensor}

    def far_peer(dy):
        return lax.rem(y + dy, n_far) * 2 + core

    kv_col = lax.div(t * heads_dev, group) * HD

    def kv_loads():
        for g in range(kv_dev):
            for which, src in ((0, k_hbm), (1, v_hbm)):
                col = pl.multiple_of(kv_col + g * HD, HD)
                yield pltpu.make_async_copy(
                    src.at[0, :, pl.ds(col, HD)],
                    kv_buf.at[z, g, which],
                    kv_load_sem.at[g, which],
                )

    for copy in kv_loads():
        copy.start()
    q_copy = pltpu.make_async_copy(q_hbm.at[0], q_buf, q_sem)
    q_copy.start()
    mask_copy = pltpu.make_async_copy(mask_ref, masks_buf.at[me], mask_load_sem)
    mask_copy.start()

    barrier = pltpu.get_barrier_semaphore()
    for k in range(1, n_masks):
        pl.semaphore_signal(barrier, inc=1, device_id=mask_peer(k))
    pl.semaphore_signal(barrier, inc=1, device_id=at(z, sibling))
    for dy in range(1, n_far):
        pl.semaphore_signal(barrier, inc=1, device_id=at(z, far_peer(dy)))

    def block_of(i):
        dy = lax.rem(lax.div(i, per_block) + 1, n_far)
        return dy, lax.rem(i, per_block), lax.rem(y + dy, n_far)

    def w_chunk(i, other):
        _, j, far_y = block_of(i)
        c = 1 - core if other else core
        return (far_y * 2 + c) * per_block + j

    def w_load(index):
        col = pl.multiple_of(index * chunk, chunk)
        return pltpu.make_async_copy(
            w_hbm.at[:, pl.ds(col, chunk)], w_buf.at[index], w_sem.at[index]
        )

    @pl.loop(0, total)
    def _(i):
        w_load(w_chunk(i, True)).start()
        w_load(w_chunk(i, False)).start()

    def kv_send(owner, g, direction):
        return pltpu.make_async_remote_copy(
            src_ref=kv_buf.at[owner, g],
            dst_ref=kv_buf.at[owner, g],
            send_sem=kv_send_sem.at[(direction + 1) // 2, owner, g],
            recv_sem=kv_recv_sem.at[owner, g],
            device_id=at(z + direction, t),
        )

    for copy in kv_loads():
        copy.wait()
    pl.semaphore_wait(barrier, n_masks + n_far - 1)

    for g in range(kv_dev):
        for direction in (1, -1):

            @pl.when((z + direction >= 0) & (z + direction < n_ctx))
            def _():
                kv_send(z, g, direction).start()

    mask_copy.wait()

    def mask_send(k):
        return pltpu.make_async_remote_copy(
            src_ref=masks_buf.at[me],
            dst_ref=masks_buf.at[me],
            send_sem=mask_send_sem.at[k],
            recv_sem=mask_recv_sem.at[k],
            device_id=mask_peer(k),
        )

    for k in range(1, n_masks):
        mask_send(k).start()

    lane = lax.broadcasted_iota(jnp.int32, (1, rows), 1)

    def pos_row(owner):
        first = order_ref[2 * owner]
        second = order_ref[2 * owner + 1]
        return (
            jnp.where(lane < span_rows, first, second) * span_rows
            + jnp.where(lane < span_rows, lane, lane - span_rows)
        ).astype(jnp.float32)

    def seg_row(owner):
        return seg_ref[:, pl.ds(pl.multiple_of(owner * rows, rows), rows)].astype(jnp.float32)

    diagonal = lax.broadcasted_iota(jnp.int32, (rows, rows), 0) == lax.broadcasted_iota(
        jnp.int32, (rows, rows), 1
    )

    def as_column(row):
        return jnp.sum(jnp.where(diagonal, row, 0.0), axis=1, keepdims=True)

    query_pos = as_column(pos_row(z))
    query_seg = as_column(seg_row(z))
    q_copy.wait()

    def attend(owner, first):
        allowed = (query_seg == seg_row(owner)) & (query_pos >= pos_row(owner))
        bias_buf[...] = jnp.where(allowed, 0.0, -1e30)
        ones = jnp.ones((rows, HD), jnp.bfloat16)
        for g in range(kv_dev):
            keys = kv_buf[owner, g, 0]
            wide = jnp.concatenate([kv_buf[owner, g, 1], ones], axis=1)

            @pl.loop(0, per_kv // HEADS_STEP)
            def _(step):
                for u in range(HEADS_STEP):
                    head = g * per_kv + step * HEADS_STEP + u
                    query = q_buf[:, pl.ds(pl.multiple_of(head * HD, HD), HD)]
                    scores = lax.dot_general(
                        query, keys, (((1,), (1,)), ((), ())), preferred_element_type=jnp.float32
                    )
                    scores = scores * factor + bias_buf[...]
                    top = jnp.max(scores, axis=1, keepdims=True)
                    if first:
                        best = top
                    else:
                        old = best_buf[head][:, :1]
                        best = jnp.maximum(old, top)
                        correct = jnp.exp(old - best)
                    probs = jnp.exp(scores - best).astype(jnp.bfloat16)
                    update = jnp.dot(probs, wide, preferred_element_type=jnp.float32)
                    if not first:
                        update = update + acc_buf[head] * correct
                    acc_buf[head] = update
                    best_buf[head] = jnp.broadcast_to(best, (rows, HD))

    attend(z, True)

    @pl.loop(1, n_ctx)
    def _(s):
        for g in range(kv_dev):
            for direction in (1, -1):
                owner = z - direction * s

                @pl.when((owner >= 0) & (owner < n_ctx))
                def _():
                    kv_send(owner, g, direction).wait_recv()

                    @pl.when((z + direction >= 0) & (z + direction < n_ctx))
                    def _():
                        kv_send(owner, g, direction).start()

        @pl.loop(0, 2)
        def _(side):
            owner = z - (1 - 2 * side) * s

            @pl.when((owner >= 0) & (owner < n_ctx))
            def _():
                attend(owner, False)

    for head in range(heads_dev):
        state = acc_buf[head]
        heads_buf[:, head * HD : (head + 1) * HD] = (state[:, :HD] / state[:, HD:]).astype(
            jnp.bfloat16
        )

    def sib_copy(i):
        return pltpu.make_async_remote_copy(
            src_ref=sib_send.at[i],
            dst_ref=sib_recv.at[i],
            send_sem=sib_send_sem.at[i],
            recv_sem=sib_recv_sem.at[i],
            device_id=at(z, sibling),
        )

    def far_copy(i):
        dy, _, _ = block_of(i)
        return pltpu.make_async_remote_copy(
            src_ref=far_send.at[i],
            dst_ref=far_recv.at[i],
            send_sem=far_send_sem.at[i],
            recv_sem=far_recv_sem.at[i],
            device_id=at(z, far_peer(dy)),
        )

    n_sent = total - per_block

    @pl.loop(0, total + LEAD)
    def _(step):
        @pl.when(step < total)
        def _():
            index = w_chunk(step, True)
            w_load(index).wait()
            sib_send[step] = jnp.dot(
                heads_buf[...], w_buf[index], preferred_element_type=jnp.float32
            ).astype(jnp.bfloat16)
            sib_copy(step).start()

        @pl.when(step >= LEAD)
        def _():
            i = step - LEAD
            index = w_chunk(i, False)
            w_load(index).wait()
            value = jnp.dot(heads_buf[...], w_buf[index], preferred_element_type=jnp.float32)
            sib_copy(i).wait_recv()
            value = value + sib_recv[i].astype(jnp.float32)

            @pl.when(i < n_sent)
            def _():
                far_send[i] = value.astype(jnp.bfloat16)
                far_copy(i).start()

            @pl.when(i >= n_sent)
            def _():
                own_buf[i - n_sent] = value

    for k in range(1, n_masks):
        mask_send(k).wait_recv()
    marks = jnp.sum(masks_buf[...].astype(jnp.float32), axis=0)
    count = jnp.sum(marks, axis=1, keepdims=True)
    mine = masks_buf[me].astype(jnp.float32)
    scale_all = float(n_dp * n_ctx * rows)
    weight = as_column(mine * scale_all / count)

    def out_copy(j):
        return pltpu.make_async_copy(
            out_buf.at[j],
            out_hbm.at[0, :, pl.ds(pl.multiple_of(j * chunk, chunk), chunk)],
            out_sem.at[j],
        )

    @pl.loop(0, per_block)
    def _(j):
        value = own_buf[j]
        for dy in range(1, n_far):
            i = (dy - 1) * per_block + j
            far_copy(i).wait_recv()
            value = value + far_recv[i].astype(jnp.float32)
        out_buf[j] = (value * weight).astype(jnp.bfloat16)
        out_copy(j).start()

    for k in range(1, n_masks):
        mask_send(k).wait_send()
    for direction in (1, -1):

        @pl.when((z + direction >= 0) & (z + direction < n_ctx))
        def _():
            @pl.loop(0, n_ctx)
            def _(s):
                owner = z - direction * s

                @pl.when((owner >= 0) & (owner < n_ctx))
                def _():
                    for g in range(kv_dev):
                        kv_send(owner, g, direction).wait_send()

    @pl.loop(0, total)
    def _(i):
        sib_copy(i).wait_send()

    @pl.loop(0, n_sent)
    def _(i):
        far_copy(i).wait_send()

    @pl.loop(0, per_block)
    def _(j):
        out_copy(j).wait()


def per_device(sizes, queries, keys, values, out_weight, segment_ids, loss_mask, span_order):
    n_dp, n_ctx, n_t = sizes
    rows = queries.shape[1]
    heads_dev = queries.shape[2] // HD
    kv_dev = max(1, heads_dev // (QH // KVH))
    depth, width = out_weight.shape
    features = width // n_t
    chunk = min(256, features)
    per_block = features // chunk
    n_far = n_t // 2
    total = n_far * per_block
    n_sent = max(1, total - per_block)
    n_masks = n_dp * n_ctx
    bf16, f32 = jnp.bfloat16, jnp.float32
    dma = pltpu.SemaphoreType.DMA
    anywhere = pl.BlockSpec(memory_space=pl.ANY)
    vmem = pl.BlockSpec(memory_space=pltpu.VMEM)
    return pl.pallas_call(
        functools.partial(kernel, sizes),
        out_shape=jax.ShapeDtypeStruct((1, rows, features), bf16),
        in_specs=[
            anywhere,
            anywhere,
            anywhere,
            anywhere,
            vmem,
            anywhere,
            pl.BlockSpec(memory_space=pltpu.SMEM),
        ],
        out_specs=anywhere,
        scratch_shapes=[
            pltpu.VMEM((rows, heads_dev * HD), bf16),
            pltpu.VMEM((n_ctx, kv_dev, 2, rows, HD), bf16),
            pltpu.VMEM((width // chunk, depth, chunk), bf16),
            pltpu.VMEM((heads_dev, rows, HD), f32),
            pltpu.VMEM((heads_dev, rows, 2 * HD), f32),
            pltpu.VMEM((rows, heads_dev * HD), bf16),
            pltpu.VMEM((rows, rows), f32),
            pltpu.VMEM((n_masks, 1, rows), jnp.int32),
            pltpu.VMEM((total, rows, chunk), bf16),
            pltpu.VMEM((total, rows, chunk), bf16),
            pltpu.VMEM((n_sent, rows, chunk), bf16),
            pltpu.VMEM((n_sent, rows, chunk), bf16),
            pltpu.VMEM((per_block, rows, chunk), f32),
            pltpu.VMEM((per_block, rows, chunk), bf16),
            dma,
            dma((kv_dev, 2)),
            dma((width // chunk,)),
            dma((2, n_ctx, kv_dev)),
            dma((n_ctx, kv_dev)),
            dma((n_masks,)),
            dma((n_masks,)),
            dma,
            dma((total,)),
            dma((total,)),
            dma((n_sent,)),
            dma((n_sent,)),
            dma((per_block,)),
        ],
        compiler_params=pltpu.CompilerParams(
            collective_id=0, has_side_effects=True, vmem_limit_bytes=62 * 1024 * 1024
        ),
    )(queries, keys, values, out_weight, segment_ids, loss_mask, span_order)


def solution(mesh):
    sizes = (mesh.shape["dp"], mesh.shape["context"], mesh.shape["tensor"])
    in_specs = (
        P("dp", "context", "tensor"),
        P("dp", "context", None),
        P("dp", "context", None),
        P("tensor", None),
        P("dp", None),
        P("dp", "context"),
        P(),
    )
    out_specs = P("dp", "context", "tensor")
    return jax.shard_map(
        functools.partial(per_device, sizes),
        mesh=mesh,
        in_specs=in_specs,
        out_specs=out_specs,
        check_vma=False,
    )
```

```python
import functools
import math

import jax
import jax.numpy as jnp
from jax import lax
from jax.experimental import pallas as pl
from jax.experimental.pallas import tpu as pltpu
from jax.sharding import PartitionSpec as P

QH = 64
KVH = 8
HD = 128
LEAD = 2
HEADS_STEP = 4
ONES = 16


def kernel(
    sizes,
    q_hbm,
    k_hbm,
    v_hbm,
    w_hbm,
    seg_ref,
    mask_ref,
    order_ref,
    out_ref,
    q_buf,
    qt_buf,
    vt_buf,
    kv_buf,
    w_buf,
    best_buf,
    acc_buf,
    heads_buf,
    bias_buf,
    masks_buf,
    sib_send,
    sib_recv,
    far_send,
    far_recv,
    own_buf,
    q_sem,
    kv_load_sem,
    w_sem,
    kv_send_sem,
    kv_recv_sem,
    mask_send_sem,
    mask_recv_sem,
    mask_load_sem,
    sib_send_sem,
    sib_recv_sem,
    far_send_sem,
    far_recv_sem,
):
    n_dp, n_ctx, n_t = sizes
    rows = q_hbm.shape[1]
    span_rows = rows // 2
    heads_dev = q_hbm.shape[2] // HD
    group = QH // KVH
    kv_dev = kv_buf.shape[1]
    per_kv = heads_dev // kv_dev
    chunk = w_buf.shape[2]
    n_far = n_t // 2
    features = w_hbm.shape[1] // n_t
    per_block = features // chunk
    total = n_far * per_block
    n_masks = n_dp * n_ctx
    factor = HD ** (-0.5) * math.log2(math.e)

    dp = lax.axis_index("dp")
    z = lax.axis_index("context")
    t = lax.axis_index("tensor")
    core = lax.rem(t, 2)
    y = lax.div(t, 2)
    sibling = t + 1 - 2 * core
    me = dp * n_ctx + z

    def mask_peer(k):
        index = lax.rem(me + k, n_masks)
        return {"dp": lax.div(index, n_ctx), "context": lax.rem(index, n_ctx), "tensor": t}

    def at(ctx, tensor):
        return {"dp": dp, "context": ctx, "tensor": tensor}

    def far_peer(dy):
        return lax.rem(y + dy, n_far) * 2 + core

    kv_col = lax.div(t * heads_dev, group) * HD

    def kv_loads():
        for g in range(kv_dev):
            for which, src in ((0, k_hbm), (1, v_hbm)):
                col = pl.multiple_of(kv_col + g * HD, HD)
                yield pltpu.make_async_copy(
                    src.at[0, :, pl.ds(col, HD)],
                    kv_buf.at[z, g, which],
                    kv_load_sem.at[g, which],
                )

    for copy in kv_loads():
        copy.start()
    q_copy = pltpu.make_async_copy(q_hbm.at[0], q_buf, q_sem)
    q_copy.start()
    mask_copy = pltpu.make_async_copy(mask_ref, masks_buf.at[me], mask_load_sem)
    mask_copy.start()

    barrier = pltpu.get_barrier_semaphore()
    for k in range(1, n_masks):
        pl.semaphore_signal(barrier, inc=1, device_id=mask_peer(k))
    pl.semaphore_signal(barrier, inc=1, device_id=at(z, sibling))
    for dy in range(1, n_far):
        pl.semaphore_signal(barrier, inc=1, device_id=at(z, far_peer(dy)))

    def block_of(i):
        dy = lax.rem(lax.div(i, per_block) + 1, n_far)
        return dy, lax.rem(i, per_block), lax.rem(y + dy, n_far)

    def w_chunk(i, other):
        _, j, far_y = block_of(i)
        c = 1 - core if other else core
        return (far_y * 2 + c) * per_block + j

    def w_load(index):
        col = pl.multiple_of(index * chunk, chunk)
        return pltpu.make_async_copy(
            w_hbm.at[:, pl.ds(col, chunk)], w_buf.at[index], w_sem.at[index]
        )

    @pl.loop(0, total)
    def _(i):
        w_load(w_chunk(i, True)).start()
        w_load(w_chunk(i, False)).start()

    def kv_send(owner, g, direction):
        return pltpu.make_async_remote_copy(
            src_ref=kv_buf.at[owner, g],
            dst_ref=kv_buf.at[owner, g],
            send_sem=kv_send_sem.at[(direction + 1) // 2, owner, g],
            recv_sem=kv_recv_sem.at[owner, g],
            device_id=at(z + direction, t),
        )

    for copy in kv_loads():
        copy.wait()
    pl.semaphore_wait(barrier, n_masks + n_far - 1)

    for g in range(kv_dev):
        for direction in (1, -1):

            @pl.when((z + direction >= 0) & (z + direction < n_ctx))
            def _():
                kv_send(z, g, direction).start()

    mask_copy.wait()

    def mask_send(k):
        return pltpu.make_async_remote_copy(
            src_ref=masks_buf.at[me],
            dst_ref=masks_buf.at[me],
            send_sem=mask_send_sem.at[k],
            recv_sem=mask_recv_sem.at[k],
            device_id=mask_peer(k),
        )

    for k in range(1, n_masks):
        mask_send(k).start()

    lane = lax.broadcasted_iota(jnp.int32, (1, rows), 1)

    def pos_row(owner):
        first = order_ref[2 * owner]
        second = order_ref[2 * owner + 1]
        return (
            jnp.where(lane < span_rows, first, second) * span_rows
            + jnp.where(lane < span_rows, lane, lane - span_rows)
        ).astype(jnp.float32)

    def seg_row(owner):
        return seg_ref[:, pl.ds(pl.multiple_of(owner * rows, rows), rows)].astype(jnp.float32)

    diagonal = lax.broadcasted_iota(jnp.int32, (rows, rows), 0) == lax.broadcasted_iota(
        jnp.int32, (rows, rows), 1
    )

    def as_column(row):
        return jnp.sum(jnp.where(diagonal, row, 0.0), axis=1, keepdims=True)

    query_pos = pos_row(z)
    query_seg = seg_row(z)
    q_copy.wait()

    @pl.loop(0, heads_dev)
    def _(head):
        part = q_buf[:, pl.ds(pl.multiple_of(head * HD, HD), HD)]
        qt_buf[head] = jnp.transpose(part, (1, 0))

    def attend(owner, first):
        key_seg = as_column(seg_row(owner))
        key_pos = as_column(pos_row(owner))
        allowed = (key_seg == query_seg) & (query_pos >= key_pos)
        bias_buf[...] = jnp.where(allowed, 0.0, -1e30)
        for g in range(kv_dev):
            vt_buf[g, :HD] = jnp.transpose(kv_buf[owner, g, 1], (1, 0))
            vt_buf[g, HD:] = jnp.ones((ONES, rows), jnp.bfloat16)

        @pl.loop(0, heads_dev // HEADS_STEP)
        def _(step):
            for u in range(HEADS_STEP):
                head = step * HEADS_STEP + u
                g = lax.div(head, per_kv)
                scores = jnp.dot(
                    kv_buf[owner, g, 0], qt_buf[head], preferred_element_type=jnp.float32
                )
                scores = scores + bias_buf[...]
                best = jnp.max(scores, axis=0, keepdims=True)
                if not first:
                    old = best_buf[head]
                    best = jnp.maximum(old, best)
                    correct = jnp.exp2((old - best) * factor)
                probs = jnp.exp2((scores - best) * factor).astype(jnp.bfloat16)
                update = jnp.dot(vt_buf[g], probs, preferred_element_type=jnp.float32)
                if not first:
                    update = update + acc_buf[head] * correct
                acc_buf[head] = update
                best_buf[head] = best

    attend(z, True)

    @pl.loop(1, n_ctx)
    def _(s):
        for g in range(kv_dev):
            for direction in (1, -1):
                owner = z - direction * s

                @pl.when((owner >= 0) & (owner < n_ctx))
                def _():
                    kv_send(owner, g, direction).wait_recv()

                    @pl.when((z + direction >= 0) & (z + direction < n_ctx))
                    def _():
                        kv_send(owner, g, direction).start()

        @pl.loop(0, 2)
        def _(side):
            owner = z - (1 - 2 * side) * s

            @pl.when((owner >= 0) & (owner < n_ctx))
            def _():
                attend(owner, False)

    for head in range(heads_dev):
        mixed = acc_buf[head, :HD] / acc_buf[head, HD : HD + 1]
        heads_buf[:, head * HD : (head + 1) * HD] = jnp.transpose(
            mixed.astype(jnp.bfloat16), (1, 0)
        )

    def sib_copy(i):
        return pltpu.make_async_remote_copy(
            src_ref=sib_send.at[i],
            dst_ref=sib_recv.at[i],
            send_sem=sib_send_sem.at[i],
            recv_sem=sib_recv_sem.at[i],
            device_id=at(z, sibling),
        )

    def far_copy(i):
        dy, _, _ = block_of(i)
        return pltpu.make_async_remote_copy(
            src_ref=far_send.at[i],
            dst_ref=far_recv.at[i],
            send_sem=far_send_sem.at[i],
            recv_sem=far_recv_sem.at[i],
            device_id=at(z, far_peer(dy)),
        )

    n_sent = total - per_block

    @pl.loop(0, total + LEAD)
    def _(step):
        @pl.when(step < total)
        def _():
            index = w_chunk(step, True)
            w_load(index).wait()
            sib_send[step] = jnp.dot(
                heads_buf[...], w_buf[index], preferred_element_type=jnp.float32
            ).astype(jnp.bfloat16)
            sib_copy(step).start()

        @pl.when(step >= LEAD)
        def _():
            i = step - LEAD
            index = w_chunk(i, False)
            w_load(index).wait()
            value = jnp.dot(heads_buf[...], w_buf[index], preferred_element_type=jnp.float32)
            sib_copy(i).wait_recv()
            value = value + sib_recv[i].astype(jnp.float32)

            @pl.when(i < n_sent)
            def _():
                far_send[i] = value.astype(jnp.bfloat16)
                far_copy(i).start()

            @pl.when(i >= n_sent)
            def _():
                own_buf[i - n_sent] = value

    for k in range(1, n_masks):
        mask_send(k).wait_recv()
    marks = jnp.sum(masks_buf[...].astype(jnp.float32), axis=0)
    count = jnp.sum(marks, axis=1, keepdims=True)
    mine = masks_buf[me].astype(jnp.float32)
    scale_all = float(n_dp * n_ctx * rows)
    weight = as_column(mine * scale_all / count)

    @pl.loop(0, per_block)
    def _(j):
        value = own_buf[j]
        for dy in range(1, n_far):
            i = (dy - 1) * per_block + j
            far_copy(i).wait_recv()
            value = value + far_recv[i].astype(jnp.float32)
        col = pl.multiple_of(j * chunk, chunk)
        out_ref[0, :, pl.ds(col, chunk)] = (value * weight).astype(jnp.bfloat16)

    for k in range(1, n_masks):
        mask_send(k).wait_send()
    for direction in (1, -1):

        @pl.when((z + direction >= 0) & (z + direction < n_ctx))
        def _():
            @pl.loop(0, n_ctx)
            def _(s):
                owner = z - direction * s

                @pl.when((owner >= 0) & (owner < n_ctx))
                def _():
                    for g in range(kv_dev):
                        kv_send(owner, g, direction).wait_send()

    @pl.loop(0, total)
    def _(i):
        sib_copy(i).wait_send()

    @pl.loop(0, n_sent)
    def _(i):
        far_copy(i).wait_send()


def per_device(sizes, queries, keys, values, out_weight, segment_ids, loss_mask, span_order):
    n_dp, n_ctx, n_t = sizes
    rows = queries.shape[1]
    heads_dev = queries.shape[2] // HD
    kv_dev = max(1, heads_dev // (QH // KVH))
    depth, width = out_weight.shape
    features = width // n_t
    chunk = min(256, features)
    per_block = features // chunk
    n_far = n_t // 2
    total = n_far * per_block
    n_sent = max(1, total - per_block)
    n_masks = n_dp * n_ctx
    bf16, f32 = jnp.bfloat16, jnp.float32
    dma = pltpu.SemaphoreType.DMA
    anywhere = pl.BlockSpec(memory_space=pl.ANY)
    vmem = pl.BlockSpec(memory_space=pltpu.VMEM)
    return pl.pallas_call(
        functools.partial(kernel, sizes),
        out_shape=pltpu.VMEM((1, rows, features), bf16),
        in_specs=[
            anywhere,
            anywhere,
            anywhere,
            anywhere,
            vmem,
            anywhere,
            pl.BlockSpec(memory_space=pltpu.SMEM),
        ],
        out_specs=vmem,
        scratch_shapes=[
            pltpu.VMEM((rows, heads_dev * HD), bf16),
            pltpu.VMEM((heads_dev, HD, rows), bf16),
            pltpu.VMEM((kv_dev, HD + ONES, rows), bf16),
            pltpu.VMEM((n_ctx, kv_dev, 2, rows, HD), bf16),
            pltpu.VMEM((width // chunk, depth, chunk), bf16),
            pltpu.VMEM((heads_dev, 1, rows), f32),
            pltpu.VMEM((heads_dev, HD + ONES, rows), f32),
            pltpu.VMEM((rows, heads_dev * HD), bf16),
            pltpu.VMEM((rows, rows), f32),
            pltpu.VMEM((n_masks, 1, rows), jnp.int32),
            pltpu.VMEM((total, rows, chunk), bf16),
            pltpu.VMEM((total, rows, chunk), bf16),
            pltpu.VMEM((n_sent, rows, chunk), bf16),
            pltpu.VMEM((n_sent, rows, chunk), bf16),
            pltpu.VMEM((per_block, rows, chunk), f32),
            dma,
            dma((kv_dev, 2)),
            dma((width // chunk,)),
            dma((2, n_ctx, kv_dev)),
            dma((n_ctx, kv_dev)),
            dma((n_masks,)),
            dma((n_masks,)),
            dma,
            dma((total,)),
            dma((total,)),
            dma((n_sent,)),
            dma((n_sent,)),
        ],
        compiler_params=pltpu.CompilerParams(
            collective_id=0, has_side_effects=True, vmem_limit_bytes=60 * 1024 * 1024
        ),
    )(queries, keys, values, out_weight, segment_ids, loss_mask, span_order)


def solution(mesh):
    sizes = (mesh.shape["dp"], mesh.shape["context"], mesh.shape["tensor"])
    in_specs = (
        P("dp", "context", "tensor"),
        P("dp", "context", None),
        P("dp", "context", None),
        P("tensor", None),
        P("dp", None),
        P("dp", "context"),
        P(),
    )
    out_specs = P("dp", "context", "tensor")
    return jax.shard_map(
        functools.partial(per_device, sizes),
        mesh=mesh,
        in_specs=in_specs,
        out_specs=out_specs,
        check_vma=False,
    )
```

```python
import functools
import math

import jax
import jax.numpy as jnp
from jax import lax
from jax.experimental import pallas as pl
from jax.experimental.pallas import tpu as pltpu
from jax.sharding import PartitionSpec as P

QH = 64
KVH = 8
HD = 128
LEAD = 2
HEADS_STEP = 8
ONES = 16


def kernel(
    sizes,
    q_hbm,
    k_hbm,
    v_hbm,
    w_hbm,
    seg_ref,
    mask_ref,
    order_ref,
    out_ref,
    q_buf,
    qt_buf,
    vt_buf,
    kv_buf,
    w_buf,
    best_buf,
    acc_buf,
    heads_buf,
    bias_buf,
    masks_buf,
    sib_send,
    sib_recv,
    far_send,
    far_recv,
    own_buf,
    q_sem,
    kv_load_sem,
    w_sem,
    kv_send_sem,
    kv_recv_sem,
    mask_send_sem,
    mask_recv_sem,
    mask_load_sem,
    sib_send_sem,
    sib_recv_sem,
    far_send_sem,
    far_recv_sem,
):
    n_dp, n_ctx, n_t = sizes
    rows = q_hbm.shape[1]
    span_rows = rows // 2
    heads_dev = q_hbm.shape[2] // HD
    group = QH // KVH
    kv_dev = kv_buf.shape[1]
    per_kv = heads_dev // kv_dev
    together = min(HEADS_STEP, heads_dev)
    chunk = w_buf.shape[2]
    n_far = n_t // 2
    features = w_hbm.shape[1] // n_t
    per_block = features // chunk
    total = n_far * per_block
    n_masks = n_dp * n_ctx
    factor = HD ** (-0.5) * math.log2(math.e)

    dp = lax.axis_index("dp")
    z = lax.axis_index("context")
    t = lax.axis_index("tensor")
    core = lax.rem(t, 2)
    y = lax.div(t, 2)
    sibling = t + 1 - 2 * core
    me = dp * n_ctx + z

    def mask_peer(k):
        index = lax.rem(me + k, n_masks)
        return {"dp": lax.div(index, n_ctx), "context": lax.rem(index, n_ctx), "tensor": t}

    def at(ctx, tensor):
        return {"dp": dp, "context": ctx, "tensor": tensor}

    def far_peer(dy):
        return lax.rem(y + dy, n_far) * 2 + core

    kv_col = lax.div(t * heads_dev, group) * HD

    def kv_loads():
        for g in range(kv_dev):
            for which, src in ((0, k_hbm), (1, v_hbm)):
                col = pl.multiple_of(kv_col + g * HD, HD)
                yield pltpu.make_async_copy(
                    src.at[0, :, pl.ds(col, HD)],
                    kv_buf.at[z, g, which],
                    kv_load_sem.at[g, which],
                )

    for copy in kv_loads():
        copy.start()
    q_copy = pltpu.make_async_copy(q_hbm.at[0], q_buf, q_sem)
    q_copy.start()
    mask_copy = pltpu.make_async_copy(mask_ref, masks_buf.at[me], mask_load_sem)
    mask_copy.start()

    barrier = pltpu.get_barrier_semaphore()
    for k in range(1, n_masks):
        pl.semaphore_signal(barrier, inc=1, device_id=mask_peer(k))
    pl.semaphore_signal(barrier, inc=1, device_id=at(z, sibling))
    for dy in range(1, n_far):
        pl.semaphore_signal(barrier, inc=1, device_id=at(z, far_peer(dy)))

    def block_of(i):
        dy = lax.rem(lax.div(i, per_block) + 1, n_far)
        return dy, lax.rem(i, per_block), lax.rem(y + dy, n_far)

    def w_chunk(i, other):
        _, j, far_y = block_of(i)
        c = 1 - core if other else core
        return (far_y * 2 + c) * per_block + j

    def w_load(index):
        col = pl.multiple_of(index * chunk, chunk)
        return pltpu.make_async_copy(
            w_hbm.at[:, pl.ds(col, chunk)], w_buf.at[index], w_sem.at[index]
        )

    @pl.loop(0, total)
    def _(i):
        w_load(w_chunk(i, True)).start()
        w_load(w_chunk(i, False)).start()

    def kv_send(owner, g, direction):
        return pltpu.make_async_remote_copy(
            src_ref=kv_buf.at[owner, g],
            dst_ref=kv_buf.at[owner, g],
            send_sem=kv_send_sem.at[(direction + 1) // 2, owner, g],
            recv_sem=kv_recv_sem.at[owner, g],
            device_id=at(z + direction, t),
        )

    for copy in kv_loads():
        copy.wait()
    pl.semaphore_wait(barrier, n_masks + n_far - 1)

    for g in range(kv_dev):
        for direction in (1, -1):

            @pl.when((z + direction >= 0) & (z + direction < n_ctx))
            def _():
                kv_send(z, g, direction).start()

    mask_copy.wait()

    def mask_send(k):
        return pltpu.make_async_remote_copy(
            src_ref=masks_buf.at[me],
            dst_ref=masks_buf.at[me],
            send_sem=mask_send_sem.at[k],
            recv_sem=mask_recv_sem.at[k],
            device_id=mask_peer(k),
        )

    for k in range(1, n_masks):
        mask_send(k).start()

    lane = lax.broadcasted_iota(jnp.int32, (1, rows), 1)

    def pos_row(owner):
        first = order_ref[2 * owner]
        second = order_ref[2 * owner + 1]
        return (
            jnp.where(lane < span_rows, first, second) * span_rows
            + jnp.where(lane < span_rows, lane, lane - span_rows)
        ).astype(jnp.float32)

    def seg_row(owner):
        return seg_ref[:, pl.ds(pl.multiple_of(owner * rows, rows), rows)].astype(jnp.float32)

    diagonal = lax.broadcasted_iota(jnp.int32, (rows, rows), 0) == lax.broadcasted_iota(
        jnp.int32, (rows, rows), 1
    )

    def as_column(row):
        return jnp.sum(jnp.where(diagonal, row, 0.0), axis=1, keepdims=True)

    query_pos = pos_row(z)
    query_seg = seg_row(z)
    q_copy.wait()

    @pl.loop(0, heads_dev)
    def _(head):
        part = q_buf[:, pl.ds(pl.multiple_of(head * HD, HD), HD)]
        qt_buf[head] = jnp.transpose(part, (1, 0))

    def attend(owner, first):
        key_seg = as_column(seg_row(owner))
        key_pos = as_column(pos_row(owner))
        allowed = (key_seg == query_seg) & (query_pos >= key_pos)
        bias_buf[...] = jnp.where(allowed, 0.0, -1e30)
        for g in range(kv_dev):
            vt_buf[g, :HD] = jnp.transpose(kv_buf[owner, g, 1], (1, 0))
            vt_buf[g, HD:] = jnp.ones((ONES, rows), jnp.bfloat16)

        @pl.loop(0, heads_dev // together)
        def _(step):
            heads = [step * together + u for u in range(together)]
            kv_heads = [lax.div(head, per_kv) for head in heads]
            bias = bias_buf[...]
            scores = [
                jnp.dot(kv_buf[owner, g, 0], qt_buf[head], preferred_element_type=jnp.float32)
                + bias
                for head, g in zip(heads, kv_heads)
            ]
            best = [jnp.max(each, axis=0, keepdims=True) for each in scores]
            if not first:
                old = [best_buf[head] for head in heads]
                best = [jnp.maximum(was, now) for was, now in zip(old, best)]
                correct = [jnp.exp2((was - now) * factor) for was, now in zip(old, best)]
            probs = [
                jnp.exp2((each - top) * factor).astype(jnp.bfloat16)
                for each, top in zip(scores, best)
            ]
            update = [
                jnp.dot(vt_buf[g], each, preferred_element_type=jnp.float32)
                for g, each in zip(kv_heads, probs)
            ]
            if not first:
                update = [
                    each + acc_buf[head] * scale
                    for head, each, scale in zip(heads, update, correct)
                ]
            for head, each, top in zip(heads, update, best):
                acc_buf[head] = each
                best_buf[head] = top

    attend(z, True)

    @pl.loop(1, n_ctx)
    def _(s):
        for g in range(kv_dev):
            for direction in (1, -1):
                owner = z - direction * s

                @pl.when((owner >= 0) & (owner < n_ctx))
                def _():
                    kv_send(owner, g, direction).wait_recv()

                    @pl.when((z + direction >= 0) & (z + direction < n_ctx))
                    def _():
                        kv_send(owner, g, direction).start()

        @pl.loop(0, 2)
        def _(side):
            owner = z - (1 - 2 * side) * s

            @pl.when((owner >= 0) & (owner < n_ctx))
            def _():
                attend(owner, False)

    for head in range(heads_dev):
        mixed = acc_buf[head, :HD] / acc_buf[head, HD : HD + 1]
        heads_buf[:, head * HD : (head + 1) * HD] = jnp.transpose(
            mixed.astype(jnp.bfloat16), (1, 0)
        )

    def sib_copy(i):
        return pltpu.make_async_remote_copy(
            src_ref=sib_send.at[i],
            dst_ref=sib_recv.at[i],
            send_sem=sib_send_sem.at[i],
            recv_sem=sib_recv_sem.at[i],
            device_id=at(z, sibling),
        )

    def far_copy(i):
        dy, _, _ = block_of(i)
        return pltpu.make_async_remote_copy(
            src_ref=far_send.at[i],
            dst_ref=far_recv.at[i],
            send_sem=far_send_sem.at[i],
            recv_sem=far_recv_sem.at[i],
            device_id=at(z, far_peer(dy)),
        )

    n_sent = total - per_block

    @pl.loop(0, total + LEAD)
    def _(step):
        @pl.when(step < total)
        def _():
            index = w_chunk(step, True)
            w_load(index).wait()
            sib_send[step] = jnp.dot(
                heads_buf[...], w_buf[index], preferred_element_type=jnp.float32
            ).astype(jnp.bfloat16)
            sib_copy(step).start()

        @pl.when(step >= LEAD)
        def _():
            i = step - LEAD
            index = w_chunk(i, False)
            w_load(index).wait()
            value = jnp.dot(heads_buf[...], w_buf[index], preferred_element_type=jnp.float32)
            sib_copy(i).wait_recv()
            value = value + sib_recv[i].astype(jnp.float32)

            @pl.when(i < n_sent)
            def _():
                far_send[i] = value.astype(jnp.bfloat16)
                far_copy(i).start()

            @pl.when(i >= n_sent)
            def _():
                own_buf[i - n_sent] = value

    for k in range(1, n_masks):
        mask_send(k).wait_recv()
    marks = jnp.sum(masks_buf[...].astype(jnp.float32), axis=0)
    count = jnp.sum(marks, axis=1, keepdims=True)
    mine = masks_buf[me].astype(jnp.float32)
    scale_all = float(n_dp * n_ctx * rows)
    weight = as_column(mine * scale_all / count)

    @pl.loop(0, per_block)
    def _(j):
        value = own_buf[j]
        for dy in range(1, n_far):
            i = (dy - 1) * per_block + j
            far_copy(i).wait_recv()
            value = value + far_recv[i].astype(jnp.float32)
        col = pl.multiple_of(j * chunk, chunk)
        out_ref[0, :, pl.ds(col, chunk)] = (value * weight).astype(jnp.bfloat16)

    for k in range(1, n_masks):
        mask_send(k).wait_send()
    for direction in (1, -1):

        @pl.when((z + direction >= 0) & (z + direction < n_ctx))
        def _():
            @pl.loop(0, n_ctx)
            def _(s):
                owner = z - direction * s

                @pl.when((owner >= 0) & (owner < n_ctx))
                def _():
                    for g in range(kv_dev):
                        kv_send(owner, g, direction).wait_send()

    @pl.loop(0, total)
    def _(i):
        sib_copy(i).wait_send()

    @pl.loop(0, n_sent)
    def _(i):
        far_copy(i).wait_send()


def per_device(sizes, queries, keys, values, out_weight, segment_ids, loss_mask, span_order):
    n_dp, n_ctx, n_t = sizes
    rows = queries.shape[1]
    heads_dev = queries.shape[2] // HD
    kv_dev = max(1, heads_dev // (QH // KVH))
    depth, width = out_weight.shape
    features = width // n_t
    chunk = min(256, features)
    per_block = features // chunk
    n_far = n_t // 2
    total = n_far * per_block
    n_sent = max(1, total - per_block)
    n_masks = n_dp * n_ctx
    bf16, f32 = jnp.bfloat16, jnp.float32
    dma = pltpu.SemaphoreType.DMA
    anywhere = pl.BlockSpec(memory_space=pl.ANY)
    vmem = pl.BlockSpec(memory_space=pltpu.VMEM)
    return pl.pallas_call(
        functools.partial(kernel, sizes),
        out_shape=pltpu.VMEM((1, rows, features), bf16),
        in_specs=[
            anywhere,
            anywhere,
            anywhere,
            anywhere,
            vmem,
            anywhere,
            pl.BlockSpec(memory_space=pltpu.SMEM),
        ],
        out_specs=vmem,
        scratch_shapes=[
            pltpu.VMEM((rows, heads_dev * HD), bf16),
            pltpu.VMEM((heads_dev, HD, rows), bf16),
            pltpu.VMEM((kv_dev, HD + ONES, rows), bf16),
            pltpu.VMEM((n_ctx, kv_dev, 2, rows, HD), bf16),
            pltpu.VMEM((width // chunk, depth, chunk), bf16),
            pltpu.VMEM((heads_dev, 1, rows), f32),
            pltpu.VMEM((heads_dev, HD + ONES, rows), f32),
            pltpu.VMEM((rows, heads_dev * HD), bf16),
            pltpu.VMEM((rows, rows), f32),
            pltpu.VMEM((n_masks, 1, rows), jnp.int32),
            pltpu.VMEM((total, rows, chunk), bf16),
            pltpu.VMEM((total, rows, chunk), bf16),
            pltpu.VMEM((n_sent, rows, chunk), bf16),
            pltpu.VMEM((n_sent, rows, chunk), bf16),
            pltpu.VMEM((per_block, rows, chunk), f32),
            dma,
            dma((kv_dev, 2)),
            dma((width // chunk,)),
            dma((2, n_ctx, kv_dev)),
            dma((n_ctx, kv_dev)),
            dma((n_masks,)),
            dma((n_masks,)),
            dma,
            dma((total,)),
            dma((total,)),
            dma((n_sent,)),
            dma((n_sent,)),
        ],
        compiler_params=pltpu.CompilerParams(
            collective_id=0, has_side_effects=True, vmem_limit_bytes=60 * 1024 * 1024
        ),
    )(queries, keys, values, out_weight, segment_ids, loss_mask, span_order)


def solution(mesh):
    sizes = (mesh.shape["dp"], mesh.shape["context"], mesh.shape["tensor"])
    in_specs = (
        P("dp", "context", "tensor"),
        P("dp", "context", None),
        P("dp", "context", None),
        P("tensor", None),
        P("dp", None),
        P("dp", "context"),
        P(),
    )
    out_specs = P("dp", "context", "tensor")
    return jax.shard_map(
        functools.partial(per_device, sizes),
        mesh=mesh,
        in_specs=in_specs,
        out_specs=out_specs,
        check_vma=False,
    )
```

```python
import functools
import math

import jax
import jax.numpy as jnp
from jax import lax
from jax.experimental import pallas as pl
from jax.experimental.pallas import tpu as pltpu
from jax.sharding import PartitionSpec as P

QH = 64
KVH = 8
HD = 128
LEAD = 2
HEADS_STEP = 16
ONES = 16


def kernel(
    sizes,
    q_hbm,
    k_hbm,
    v_hbm,
    w_hbm,
    seg_ref,
    mask_ref,
    order_ref,
    out_ref,
    q_buf,
    qt_buf,
    vt_buf,
    kv_buf,
    w_buf,
    best_buf,
    acc_buf,
    heads_buf,
    bias_buf,
    masks_buf,
    sib_send,
    sib_recv,
    far_send,
    far_recv,
    own_buf,
    q_sem,
    kv_load_sem,
    w_sem,
    kv_send_sem,
    kv_recv_sem,
    mask_send_sem,
    mask_recv_sem,
    mask_load_sem,
    sib_send_sem,
    sib_recv_sem,
    far_send_sem,
    far_recv_sem,
):
    n_dp, n_ctx, n_t = sizes
    rows = q_hbm.shape[1]
    span_rows = rows // 2
    heads_dev = q_hbm.shape[2] // HD
    group = QH // KVH
    kv_dev = kv_buf.shape[1]
    per_kv = heads_dev // kv_dev
    together = min(HEADS_STEP, heads_dev)
    chunk = w_buf.shape[2]
    n_far = n_t // 2
    features = w_hbm.shape[1] // n_t
    per_block = features // chunk
    total = n_far * per_block
    n_masks = n_dp * n_ctx
    factor = HD ** (-0.5) * math.log2(math.e)

    dp = lax.axis_index("dp")
    z = lax.axis_index("context")
    t = lax.axis_index("tensor")
    core = lax.rem(t, 2)
    y = lax.div(t, 2)
    sibling = t + 1 - 2 * core
    me = dp * n_ctx + z

    def mask_peer(k):
        index = lax.rem(me + k, n_masks)
        return {"dp": lax.div(index, n_ctx), "context": lax.rem(index, n_ctx), "tensor": t}

    def at(ctx, tensor):
        return {"dp": dp, "context": ctx, "tensor": tensor}

    def far_peer(dy):
        return lax.rem(y + dy, n_far) * 2 + core

    kv_col = lax.div(t * heads_dev, group) * HD

    def kv_loads():
        for g in range(kv_dev):
            for which, src in ((0, k_hbm), (1, v_hbm)):
                col = pl.multiple_of(kv_col + g * HD, HD)
                yield pltpu.make_async_copy(
                    src.at[0, :, pl.ds(col, HD)],
                    kv_buf.at[z, g, which],
                    kv_load_sem.at[g, which],
                )

    for copy in kv_loads():
        copy.start()
    q_copy = pltpu.make_async_copy(q_hbm.at[0], q_buf, q_sem)
    q_copy.start()
    mask_copy = pltpu.make_async_copy(mask_ref, masks_buf.at[me], mask_load_sem)
    mask_copy.start()

    barrier = pltpu.get_barrier_semaphore()
    for k in range(1, n_masks):
        pl.semaphore_signal(barrier, inc=1, device_id=mask_peer(k))
    pl.semaphore_signal(barrier, inc=1, device_id=at(z, sibling))
    for dy in range(1, n_far):
        pl.semaphore_signal(barrier, inc=1, device_id=at(z, far_peer(dy)))

    def block_of(i):
        dy = lax.rem(lax.div(i, per_block) + 1, n_far)
        return dy, lax.rem(i, per_block), lax.rem(y + dy, n_far)

    def w_chunk(i, other):
        _, j, far_y = block_of(i)
        c = 1 - core if other else core
        return (far_y * 2 + c) * per_block + j

    def w_load(index):
        col = pl.multiple_of(index * chunk, chunk)
        return pltpu.make_async_copy(
            w_hbm.at[:, pl.ds(col, chunk)], w_buf.at[index], w_sem.at[index]
        )

    @pl.loop(0, total)
    def _(i):
        w_load(w_chunk(i, True)).start()
        w_load(w_chunk(i, False)).start()

    def kv_send(owner, g, direction):
        return pltpu.make_async_remote_copy(
            src_ref=kv_buf.at[owner, g],
            dst_ref=kv_buf.at[owner, g],
            send_sem=kv_send_sem.at[(direction + 1) // 2, owner, g],
            recv_sem=kv_recv_sem.at[owner, g],
            device_id=at(z + direction, t),
        )

    for copy in kv_loads():
        copy.wait()
    pl.semaphore_wait(barrier, n_masks + n_far - 1)

    for g in range(kv_dev):
        for direction in (1, -1):

            @pl.when((z + direction >= 0) & (z + direction < n_ctx))
            def _():
                kv_send(z, g, direction).start()

    mask_copy.wait()

    def mask_send(k):
        return pltpu.make_async_remote_copy(
            src_ref=masks_buf.at[me],
            dst_ref=masks_buf.at[me],
            send_sem=mask_send_sem.at[k],
            recv_sem=mask_recv_sem.at[k],
            device_id=mask_peer(k),
        )

    for k in range(1, n_masks):
        mask_send(k).start()

    lane = lax.broadcasted_iota(jnp.int32, (1, rows), 1)

    def pos_row(owner):
        first = order_ref[2 * owner]
        second = order_ref[2 * owner + 1]
        return (
            jnp.where(lane < span_rows, first, second) * span_rows
            + jnp.where(lane < span_rows, lane, lane - span_rows)
        ).astype(jnp.float32)

    def seg_row(owner):
        return seg_ref[:, pl.ds(pl.multiple_of(owner * rows, rows), rows)].astype(jnp.float32)

    diagonal = lax.broadcasted_iota(jnp.int32, (rows, rows), 0) == lax.broadcasted_iota(
        jnp.int32, (rows, rows), 1
    )

    def as_column(row):
        return jnp.sum(jnp.where(diagonal, row, 0.0), axis=1, keepdims=True)

    query_pos = pos_row(z)
    query_seg = seg_row(z)
    q_copy.wait()

    @pl.loop(0, heads_dev)
    def _(head):
        part = q_buf[:, pl.ds(pl.multiple_of(head * HD, HD), HD)]
        qt_buf[head] = jnp.transpose(part, (1, 0))

    def attend(owner, first):
        key_seg = as_column(seg_row(owner))
        key_pos = as_column(pos_row(owner))
        allowed = (key_seg == query_seg) & (query_pos >= key_pos)
        bias_buf[...] = jnp.where(allowed, 0.0, -1e30)
        for g in range(kv_dev):
            vt_buf[g, :HD] = jnp.transpose(kv_buf[owner, g, 1], (1, 0))
            vt_buf[g, HD:] = jnp.ones((ONES, rows), jnp.bfloat16)

        @pl.loop(0, heads_dev // together)
        def _(step):
            heads = [step * together + u for u in range(together)]
            kv_heads = [lax.div(head, per_kv) for head in heads]
            bias = bias_buf[...]
            scores = [
                jnp.dot(kv_buf[owner, g, 0], qt_buf[head], preferred_element_type=jnp.float32)
                + bias
                for head, g in zip(heads, kv_heads)
            ]
            best = [jnp.max(each, axis=0, keepdims=True) for each in scores]
            if not first:
                old = [best_buf[head] for head in heads]
                best = [jnp.maximum(was, now) for was, now in zip(old, best)]
                correct = [jnp.exp2((was - now) * factor) for was, now in zip(old, best)]
            probs = [
                jnp.exp2((each - top) * factor).astype(jnp.bfloat16)
                for each, top in zip(scores, best)
            ]
            update = [
                jnp.dot(vt_buf[g], each, preferred_element_type=jnp.float32)
                for g, each in zip(kv_heads, probs)
            ]
            if not first:
                update = [
                    each + acc_buf[head] * scale
                    for head, each, scale in zip(heads, update, correct)
                ]
            for head, each, top in zip(heads, update, best):
                acc_buf[head] = each
                best_buf[head] = top

    attend(z, True)

    def relay(s):
        for g in range(kv_dev):
            for direction in (1, -1):
                owner = z - direction * s

                @pl.when((owner >= 0) & (owner < n_ctx))
                def _():
                    kv_send(owner, g, direction).wait_recv()

                    @pl.when((z + direction >= 0) & (z + direction < n_ctx))
                    def _():
                        kv_send(owner, g, direction).start()

    relay(1)

    @pl.loop(1, n_ctx)
    def _(s):
        has_left = 1 - lax.div(s - z + n_ctx - 1, n_ctx)

        @pl.loop(0, 2)
        def _(k):
            side = k * has_left + (1 - k) * (1 - has_left)
            owner = z - (1 - 2 * side) * s

            @pl.when((owner >= 0) & (owner < n_ctx))
            def _():
                attend(owner, False)

            @pl.when((k == 0) & (s + 1 < n_ctx))
            def _():
                relay(s + 1)

    for head in range(heads_dev):
        mixed = acc_buf[head, :HD] / acc_buf[head, HD : HD + 1]
        heads_buf[:, head * HD : (head + 1) * HD] = jnp.transpose(
            mixed.astype(jnp.bfloat16), (1, 0)
        )

    def sib_copy(i):
        return pltpu.make_async_remote_copy(
            src_ref=sib_send.at[i],
            dst_ref=sib_recv.at[i],
            send_sem=sib_send_sem.at[i],
            recv_sem=sib_recv_sem.at[i],
            device_id=at(z, sibling),
        )

    def far_copy(i):
        dy, _, _ = block_of(i)
        return pltpu.make_async_remote_copy(
            src_ref=far_send.at[i],
            dst_ref=far_recv.at[i],
            send_sem=far_send_sem.at[i],
            recv_sem=far_recv_sem.at[i],
            device_id=at(z, far_peer(dy)),
        )

    n_sent = total - per_block

    @pl.loop(0, total + LEAD)
    def _(step):
        @pl.when(step < total)
        def _():
            index = w_chunk(step, True)
            w_load(index).wait()
            sib_send[step] = jnp.dot(
                heads_buf[...], w_buf[index], preferred_element_type=jnp.float32
            ).astype(jnp.bfloat16)
            sib_copy(step).start()

        @pl.when(step >= LEAD)
        def _():
            i = step - LEAD
            index = w_chunk(i, False)
            w_load(index).wait()
            value = jnp.dot(heads_buf[...], w_buf[index], preferred_element_type=jnp.float32)
            sib_copy(i).wait_recv()
            value = value + sib_recv[i].astype(jnp.float32)

            @pl.when(i < n_sent)
            def _():
                far_send[i] = value.astype(jnp.bfloat16)
                far_copy(i).start()

            @pl.when(i >= n_sent)
            def _():
                own_buf[i - n_sent] = value

    for k in range(1, n_masks):
        mask_send(k).wait_recv()
    marks = jnp.sum(masks_buf[...].astype(jnp.float32), axis=0)
    count = jnp.sum(marks, axis=1, keepdims=True)
    mine = masks_buf[me].astype(jnp.float32)
    scale_all = float(n_dp * n_ctx * rows)
    weight = as_column(mine * scale_all / count)

    @pl.loop(0, per_block)
    def _(j):
        value = own_buf[j]
        for dy in range(1, n_far):
            i = (dy - 1) * per_block + j
            far_copy(i).wait_recv()
            value = value + far_recv[i].astype(jnp.float32)
        col = pl.multiple_of(j * chunk, chunk)
        out_ref[0, :, pl.ds(col, chunk)] = (value * weight).astype(jnp.bfloat16)

    for k in range(1, n_masks):
        mask_send(k).wait_send()
    for direction in (1, -1):

        @pl.when((z + direction >= 0) & (z + direction < n_ctx))
        def _():
            @pl.loop(0, n_ctx)
            def _(s):
                owner = z - direction * s

                @pl.when((owner >= 0) & (owner < n_ctx))
                def _():
                    for g in range(kv_dev):
                        kv_send(owner, g, direction).wait_send()

    @pl.loop(0, total)
    def _(i):
        sib_copy(i).wait_send()

    @pl.loop(0, n_sent)
    def _(i):
        far_copy(i).wait_send()


def per_device(sizes, queries, keys, values, out_weight, segment_ids, loss_mask, span_order):
    n_dp, n_ctx, n_t = sizes
    rows = queries.shape[1]
    heads_dev = queries.shape[2] // HD
    kv_dev = max(1, heads_dev // (QH // KVH))
    depth, width = out_weight.shape
    features = width // n_t
    chunk = min(256, features)
    per_block = features // chunk
    n_far = n_t // 2
    total = n_far * per_block
    n_sent = max(1, total - per_block)
    n_masks = n_dp * n_ctx
    bf16, f32 = jnp.bfloat16, jnp.float32
    dma = pltpu.SemaphoreType.DMA
    anywhere = pl.BlockSpec(memory_space=pl.ANY)
    vmem = pl.BlockSpec(memory_space=pltpu.VMEM)
    return pl.pallas_call(
        functools.partial(kernel, sizes),
        out_shape=pltpu.VMEM((1, rows, features), bf16),
        in_specs=[
            anywhere,
            anywhere,
            anywhere,
            anywhere,
            vmem,
            anywhere,
            pl.BlockSpec(memory_space=pltpu.SMEM),
        ],
        out_specs=vmem,
        scratch_shapes=[
            pltpu.VMEM((rows, heads_dev * HD), bf16),
            pltpu.VMEM((heads_dev, HD, rows), bf16),
            pltpu.VMEM((kv_dev, HD + ONES, rows), bf16),
            pltpu.VMEM((n_ctx, kv_dev, 2, rows, HD), bf16),
            pltpu.VMEM((width // chunk, depth, chunk), bf16),
            pltpu.VMEM((heads_dev, 1, rows), f32),
            pltpu.VMEM((heads_dev, HD + ONES, rows), f32),
            pltpu.VMEM((rows, heads_dev * HD), bf16),
            pltpu.VMEM((rows, rows), f32),
            pltpu.VMEM((n_masks, 1, rows), jnp.int32),
            pltpu.VMEM((total, rows, chunk), bf16),
            pltpu.VMEM((total, rows, chunk), bf16),
            pltpu.VMEM((n_sent, rows, chunk), bf16),
            pltpu.VMEM((n_sent, rows, chunk), bf16),
            pltpu.VMEM((per_block, rows, chunk), f32),
            dma,
            dma((kv_dev, 2)),
            dma((width // chunk,)),
            dma((2, n_ctx, kv_dev)),
            dma((n_ctx, kv_dev)),
            dma((n_masks,)),
            dma((n_masks,)),
            dma,
            dma((total,)),
            dma((total,)),
            dma((n_sent,)),
            dma((n_sent,)),
        ],
        compiler_params=pltpu.CompilerParams(
            collective_id=0, has_side_effects=True, vmem_limit_bytes=60 * 1024 * 1024
        ),
    )(queries, keys, values, out_weight, segment_ids, loss_mask, span_order)


def solution(mesh):
    sizes = (mesh.shape["dp"], mesh.shape["context"], mesh.shape["tensor"])
    in_specs = (
        P("dp", "context", "tensor"),
        P("dp", "context", None),
        P("dp", "context", None),
        P("tensor", None),
        P("dp", None),
        P("dp", "context"),
        P(),
    )
    out_specs = P("dp", "context", "tensor")
    return jax.shard_map(
        functools.partial(per_device, sizes),
        mesh=mesh,
        in_specs=in_specs,
        out_specs=out_specs,
        check_vma=False,
    )
```
